32 devices in a mesh: lat: 8 (over y, x, core), lon: 4 (over z).
Axes of the slice: x: 2, y: 2, z: 4, core: 2. Of those that a mesh axis runs over, the one named last changes fastest.
Arguments:
- loadings: float32 [176, 720, 200], P('lat', 'lon'), may hold values from -60 to 60, as said below
Outputs:
- rotated: float32 [176, 720, 200], P('lat', 'lon')
- rotation: float32 [200, 200], replicated
The draws below stay inside these ranges and needn't reach their ends.
Inputs may be any that keep to these rules, and one draw needn't show every extreme that they name: Every grid point's loadings are not all zero.
All inputs are finite; a program needn't handle non-finite values.
Results may differ from the reference program's by a relative error of at most 0.00011.
Values sent between devices are 32-bit elements; how exact they have to be, the bound alone decides.
A program may use at most 64 MiB of HBM per device.

```python
import math
import jax
import jax.numpy as jnp
from jax import lax

K = 200
LAT_DEV = 22
SWEEPS = 2
NS_STEPS = 20
NLAT = 176
NLON = 720
N_LAT = 8


def draw_loadings(key, part):
    base_key = jax.random.fold_in(key, 17)
    keys = jax.random.split(base_key, 8)
    rows = jnp.arange(NLAT).astype(jnp.int32)[:, None]
    cols = jnp.arange(NLON).astype(jnp.int32)[None, :]
    region = rows * 10 // NLAT * 20 + cols * 20 // NLON
    order = jax.random.permutation(keys[0], K).astype(jnp.int32)
    primary = order[region % K]
    secondary = order[(region + 20 + rows % 3) % K]
    flips = jax.random.randint(keys[1], (NLAT, NLON, 1), 0, 2).astype(jnp.float32) * 2.0 - 1.0
    modes = jnp.arange(K).astype(jnp.int32)[None, None, :]
    noise = 0.25 * jnp.clip(jax.random.normal(keys[2], (NLAT, NLON, K), jnp.float32), -3.0, 3.0)
    strength = 2.0 + jnp.abs(jnp.clip(jax.random.normal(keys[3], (NLAT, NLON, 1), jnp.float32), -3.0, 3.0))
    row_scale = jnp.exp(jax.random.uniform(keys[5], (NLAT, NLON, 1), jnp.float32) * math.log(10.0))
    side = 0.5 * strength * jax.random.uniform(keys[4], (NLAT, NLON, 1), jnp.float32, -1.0, 1.0)
    structure = noise + jnp.where(modes == primary[:, :, None], flips * strength, 0.0)
    structure = structure + jnp.where(modes == secondary[:, :, None], side, 0.0)
    col_scale = jnp.exp(jax.random.uniform(keys[6], (1, 1, K), jnp.float32, -1.0, 0.0) * math.log(3.0))
    structure = structure * row_scale * col_scale
    gauss = jax.random.normal(keys[7], (K, K), jnp.float32)
    ortho, upper = jnp.linalg.qr(gauss)
    ortho = ortho * jnp.where(jnp.diagonal(upper) >= 0.0, 1.0, -1.0)[None, :]
    mixed = jnp.dot(structure.reshape(NLAT * NLON, K), ortho, precision=lax.Precision.HIGHEST)
    return jnp.clip(mixed.reshape(NLAT, NLON, K), -60.0, 60.0)


def setup_inputs(seed: int = 0) -> dict:
    key_list = jax.random.split(jax.random.key(seed), 2)
    loadings = draw_loadings(jax.random.fold_in(key_list[1], 71), 0)
    return dict(loadings=loadings)


def grid_weights():
    rows = jnp.arange(NLAT).astype(jnp.float32)
    degrees = -90.0 + (rows + 0.5) * (180.0 / NLAT)
    return jnp.cos(degrees * (math.pi / 180.0))

def matmul(left, right):
    return jnp.dot(left, right, precision=lax.Precision.HIGHEST)

def polar_factor(gradient):
    iterate = gradient / jnp.sqrt(jnp.sum(gradient * gradient))
    for count in range(NS_STEPS):
        iterate = 1.5 * iterate - 0.5 * matmul(iterate, matmul(iterate.T, iterate))
    return iterate

def reference(loadings):
    row_norm = jnp.sqrt(lax.optimization_barrier(jnp.sum(loadings * loadings, axis=-1, keepdims=True)) + 1e-06)
    normed = loadings / row_norm
    weights = grid_weights()
    total = jnp.sum(weights) * NLON
    bands = normed.reshape(N_LAT, LAT_DEV * NLON, K)
    band_weights = jnp.repeat(weights.reshape(N_LAT, LAT_DEV), NLON, axis=1).reshape(N_LAT, LAT_DEV * NLON, 1)
    rotation = jnp.eye(K, dtype=jnp.float32)
    for sweep_index in range(SWEEPS):

        def colsq_band(carry, pair):
            block, block_weights = pair
            spun = matmul(block, rotation)
            return (carry + lax.optimization_barrier(jnp.sum(block_weights * spun * spun, axis=0)), None)
        colsq, unused = lax.scan(colsq_band, jnp.zeros((K,), jnp.float32), (bands, band_weights))

        def gradient_band(carry, pair):
            block, block_weights = pair
            spun = matmul(block, rotation)
            term = block_weights * (spun * spun * spun - spun * (colsq / total)[None, :])
            return (carry + matmul(block.T, term), None)
        gradient, unused = lax.scan(gradient_band, jnp.zeros((K, K), jnp.float32), (bands, band_weights))
        rotation = polar_factor(gradient)
    flat = normed.reshape(NLAT * NLON, K)
    rotated = matmul(flat, rotation).reshape(NLAT, NLON, K) * row_norm
    return (rotated, rotation)
```

```python
import functools
import math

import jax
import jax.numpy as jnp
import numpy as np
from jax import lax
from jax.experimental import pallas as pl
from jax.experimental.pallas import tpu as pltpu
from jax.sharding import PartitionSpec as P

SWEEPS = 2
NS_STEPS = 20
SUB = 8
LANES = 256
MESH = pl.DeviceIdType.MESH
NN = (((1,), (0,)), ((), ()))
NT = (((1,), (1,)), ((), ()))


def split(value):
    high = value.astype(jnp.bfloat16)
    low = (value - high.astype(jnp.float32)).astype(jnp.bfloat16)
    return high, low


def mm(left, right, dims=NN):
    return lax.dot_general(left, right, dims, preferred_element_type=jnp.float32)


def mm3(left, right, dims=NN):
    lh, ll = left
    rh, rl = right
    return mm(lh, rh, dims) + (mm(lh, rl, dims) + mm(ll, rh, dims))


def polar(gradient):
    squares = jnp.sum(gradient * gradient, axis=0, keepdims=True)
    norm = jnp.sqrt(jnp.sum(squares, axis=1, keepdims=True))

    def step(_, x):
        parts = split(x)
        inner = mm3(parts, parts, NT)
        return 1.5 * x - 0.5 * mm3(split(inner), parts)

    return lax.fori_loop(0, NS_STEPS, step, gradient / norm)


class Reduce:
    def __init__(self, me, n, n_lon, owners, bufs, sems):
        self.me, self.n, self.n_lon, self.owners = me, n, n_lon, owners
        self.src, self.got, self.full = bufs
        self.sems = sems

    def copy(self, source, target, device, phase, sent, landed):
        return pltpu.make_async_remote_copy(
            src_ref=source,
            dst_ref=target,
            send_sem=self.sems.at[phase, sent],
            recv_sem=self.sems.at[phase + 1, landed],
            device_id=(device // self.n_lon, lax.rem(device, self.n_lon)),
            device_id_type=MESH,
        )

    def part(self, peer, source):
        return self.copy(self.src.at[peer], self.got.at[source], peer, 0, peer, source)

    def whole(self, peer, owner):
        return self.copy(self.full.at[owner], self.full.at[owner], peer, 2, peer, owner)

    def scatter(self):
        me, n = self.me, self.n
        for shift in range(1, n):
            peer = lax.rem(me + shift, n)

            @pl.when(peer < self.owners)
            def _():
                self.part(peer, me).start()

    def gather(self):
        me, n = self.me, self.n
        following = lax.rem(me + 1, n)

        @pl.when(me < self.owners)
        def _():
            acc = self.src[me]
            for shift in range(1, n):
                peer = lax.rem(me + n - shift, n)
                self.copy(self.src.at[me], self.got.at[peer], following, 0, peer, peer).wait_recv()
                acc = acc + self.got[peer]
            self.full[me] = acc
            for shift in range(1, n):
                self.whole(lax.rem(me + shift, n), me).start()

        for shift in range(1, n):
            peer = lax.rem(me + n - shift, n)

            @pl.when(peer < self.owners)
            def _():
                self.whole(following, peer).wait_recv()
                self.part(peer, me).wait_send()

        @pl.when(me < self.owners)
        def _():
            for shift in range(1, n):
                self.whole(lax.rem(me + shift, n), me).wait_send()


def kernel(n_lat, n_lon, total, weights, loadings, out, yh, yl, th, tl, gram, cubic,
           src1, got1, full1, src2, got2, full2, sems1, sems2):
    lat_rows, lon_cols, modes = loadings.shape
    n = n_lat * n_lon
    owners = modes // SUB
    lat, lon = lax.axis_index("lat"), lax.axis_index("lon")
    me = lat * n_lon + lon

    barrier = pltpu.get_barrier_semaphore()
    for shift in range(1, n):
        peer = lax.rem(me + shift, n)
        pl.semaphore_signal(barrier, inc=1, device_id=(peer // n_lon, lax.rem(peer, n_lon)),
                            device_id_type=MESH)

    gram[...] = jnp.zeros_like(gram)
    cubic[...] = jnp.zeros_like(cubic)

    def first(j, carry):
        weight = weights[0, lat * lat_rows + j]
        root = weights[1, lat * lat_rows + j]
        inverse = weights[2, lat * lat_rows + j]
        x = loadings[j]
        scale = root / jnp.sqrt(jnp.sum(x * x, axis=1, keepdims=True) + 1e-06)
        y = x * scale
        y_parts = split(y)
        t_parts = split(y.T)
        yh[j], yl[j] = y_parts
        th[j], tl[j] = t_parts
        gram[...] += mm3(t_parts, y_parts)
        cubic[...] += mm3(t_parts, split(y * y * y * inverse))
        return carry

    lax.fori_loop(0, lat_rows, first, 0)
    src1[:, 0, :, :modes] = gram[...].reshape(owners, SUB, modes)
    src1[:, 1, :, :modes] = cubic[...].reshape(owners, SUB, modes)

    pl.semaphore_wait(barrier, n - 1)
    reduce1 = Reduce(me, n, n_lon, owners, (src1, got1, full1), sems1)
    reduce1.scatter()
    reduce1.gather()
    whole = full1[:, 0, :, :modes].reshape(modes, modes)
    row = lax.broadcasted_iota(jnp.int32, (modes, modes), 0)
    col = lax.broadcasted_iota(jnp.int32, (modes, modes), 1)
    colsq = jnp.sum(jnp.where(row == col, whole, 0.0), axis=0, keepdims=True)
    gradient = full1[:, 1, :, :modes].reshape(modes, modes) - whole * (colsq / total)
    rotation = polar(gradient)

    r_parts = split(rotation)
    cubic[...] = jnp.zeros_like(cubic)

    def second(j, carry):
        inverse = weights[2, lat * lat_rows + j]
        spun = mm3((yh[j], yl[j]), r_parts)
        cubic[...] += mm3((th[j], tl[j]), split(spun * spun * spun * inverse))
        return carry

    lax.fori_loop(0, lat_rows, second, 0)
    src2[:, 0, :, :modes] = cubic[...].reshape(owners, SUB, modes)
    reduce2 = Reduce(me, n, n_lon, owners, (src2, got2, full2), sems2)
    reduce2.scatter()
    turned = mm3(split(whole), r_parts)
    colsq = jnp.sum(rotation * turned, axis=0, keepdims=True)
    reduce2.gather()
    gradient = full2[:, 0, :, :modes].reshape(modes, modes) - turned * (colsq / total)
    out[...] = polar(gradient)


def latitude_weight(lat_total):
    rows = np.arange(lat_total, dtype=np.float32)
    degrees = np.float32(-90.0) + (rows + np.float32(0.5)) * np.float32(180.0 / lat_total)
    return np.cos(degrees * np.float32(math.pi / 180.0)).astype(np.float32)


def shards(n_lat, n_lon, loadings):
    lat_rows, lon_cols, modes = loadings.shape
    n = n_lat * n_lon
    owners = modes // SUB
    assert modes % SUB == 0 and owners <= n and modes <= LANES
    weights = latitude_weight(lat_rows * n_lat)
    total = float(np.sum(weights, dtype=np.float32) * np.float32(lon_cols * n_lon))
    table = jnp.asarray(np.stack([weights, np.sqrt(weights), 1.0 / weights]).astype(np.float32))
    f32, bf16 = jnp.float32, jnp.bfloat16

    def bufs(parts):
        return [
            pltpu.VMEM((owners, parts, SUB, LANES), f32),
            pltpu.VMEM((n, parts, SUB, LANES), f32),
            pltpu.VMEM((owners, parts, SUB, LANES), f32),
        ]

    rotation = pl.pallas_call(
        functools.partial(kernel, n_lat, n_lon, total),
        out_shape=jax.ShapeDtypeStruct((modes, modes), f32),
        in_specs=[
            pl.BlockSpec(memory_space=pltpu.SMEM),
            pl.BlockSpec(memory_space=pltpu.VMEM),
        ],
        out_specs=pl.BlockSpec(memory_space=pltpu.VMEM),
        scratch_shapes=[
            pltpu.VMEM((lat_rows, lon_cols, modes), bf16),
            pltpu.VMEM((lat_rows, lon_cols, modes), bf16),
            pltpu.VMEM((lat_rows, modes, lon_cols), bf16),
            pltpu.VMEM((lat_rows, modes, lon_cols), bf16),
            pltpu.VMEM((modes, modes), f32),
            pltpu.VMEM((modes, modes), f32),
            *bufs(2),
            *bufs(1),
            pltpu.SemaphoreType.DMA((4, n)),
            pltpu.SemaphoreType.DMA((4, n)),
        ],
        compiler_params=pltpu.CompilerParams(
            collective_id=0, has_side_effects=True, vmem_limit_bytes=60 * 1024 * 1024
        ),
    )(table, loadings)
    rotated = jnp.einsum("abk,kl->abl", loadings, rotation, precision=lax.Precision.HIGH)
    return (rotated, rotation)


def solution(mesh):
    return jax.shard_map(
        functools.partial(shards, mesh.shape["lat"], mesh.shape["lon"]),
        mesh=mesh,
        in_specs=(P("lat", "lon", None),),
        out_specs=(P("lat", "lon", None), P()),
        check_vma=False,
    )
```

```python
import functools
import math

import jax
import jax.numpy as jnp
import numpy as np
from jax import lax
from jax.experimental import pallas as pl
from jax.experimental.pallas import tpu as pltpu
from jax.sharding import PartitionSpec as P

SWEEPS = 2
NS_STEPS = 20
SUB = 8
LANES = 256
MESH = pl.DeviceIdType.MESH
NN = (((1,), (0,)), ((), ()))
NT = (((1,), (1,)), ((), ()))


def split(value):
    high = value.astype(jnp.bfloat16)
    low = (value - high.astype(jnp.float32)).astype(jnp.bfloat16)
    return high, low


def mm(left, right, dims=NN):
    return lax.dot_general(left, right, dims, preferred_element_type=jnp.float32)


def mm3(left, right, dims=NN):
    lh, ll = left
    rh, rl = right
    return mm(lh, rh, dims) + (mm(lh, rl, dims) + mm(ll, rh, dims))


def polar(gradient):
    squares = jnp.sum(gradient * gradient, axis=0, keepdims=True)
    norm = jnp.sqrt(jnp.sum(squares, axis=1, keepdims=True))

    def step(_, x):
        parts = split(x)
        inner = mm3(parts, parts, NT)
        return 1.5 * x - 0.5 * mm3(split(inner), parts)

    return lax.fori_loop(0, NS_STEPS, step, gradient / norm)


class Reduce:
    def __init__(self, me, n, n_lon, owners, bufs, sems):
        self.me, self.n, self.n_lon, self.owners = me, n, n_lon, owners
        self.src, self.got, self.full, self.rows = bufs
        self.sems = sems

    def copy(self, source, target, device, phase, sent, landed):
        return pltpu.make_async_remote_copy(
            src_ref=source,
            dst_ref=target,
            send_sem=self.sems.at[phase, sent],
            recv_sem=self.sems.at[phase + 1, landed],
            device_id=(device // self.n_lon, lax.rem(device, self.n_lon)),
            device_id_type=MESH,
        )

    def part(self, peer, source):
        return self.copy(self.src.at[peer], self.got.at[source], peer, 0, peer, source)

    def whole(self, peer, owner):
        return self.copy(self.full.at[owner], self.full.at[owner], peer, 2, peer, owner)

    def row(self, peer, source):
        return self.copy(self.rows.at[source], self.rows.at[source], peer, 4, peer, source)

    def spread(self, value):
        me, n = self.me, self.n
        self.rows[me, :, : value.shape[1]] = value
        for shift in range(1, n):
            self.row(lax.rem(me + shift, n), me).start()

    def total(self, width):
        me, n = self.me, self.n
        for shift in range(1, n):
            peer = lax.rem(me + n - shift, n)
            self.row(peer, peer).wait_recv()
        acc = self.rows[0]
        for source in range(1, n):
            acc = acc + self.rows[source]
        for shift in range(1, n):
            self.row(lax.rem(me + shift, n), me).wait_send()
        return acc[:, :width]

    def scatter(self):
        me, n = self.me, self.n
        for shift in range(1, n):
            peer = lax.rem(me + shift, n)

            @pl.when(peer < self.owners)
            def _():
                self.part(peer, me).start()

    def gather(self):
        me, n = self.me, self.n
        following = lax.rem(me + 1, n)

        @pl.when(me < self.owners)
        def _():
            acc = self.src[me]
            for shift in range(1, n):
                peer = lax.rem(me + n - shift, n)
                self.copy(self.src.at[me], self.got.at[peer], following, 0, peer, peer).wait_recv()
                acc = acc + self.got[peer]
            self.full[me] = acc
            for shift in range(1, n):
                self.whole(lax.rem(me + shift, n), me).start()

        for shift in range(1, n):
            peer = lax.rem(me + n - shift, n)

            @pl.when(peer < self.owners)
            def _():
                self.whole(following, peer).wait_recv()
                self.part(peer, me).wait_send()

        @pl.when(me < self.owners)
        def _():
            for shift in range(1, n):
                self.whole(lax.rem(me + shift, n), me).wait_send()


def kernel(n_lat, n_lon, total, weights, loadings, out, held, yh, yl, th, tl, gram, cubic,
           src1, got1, full1, rows1, src2, got2, full2, rows2, sems1, sems2, loads):
    lat_rows, lon_cols, modes = held.shape
    n = n_lat * n_lon
    owners = modes // SUB
    unroll = 2 if lat_rows % 2 == 0 else 1
    lat, lon = lax.axis_index("lat"), lax.axis_index("lon")
    me = lat * n_lon + lon
    reduce1 = Reduce(me, n, n_lon, owners, (src1, got1, full1, rows1), sems1)
    reduce2 = Reduce(me, n, n_lon, owners, (src2, got2, full2, rows2), sems2)

    def load(j):
        return pltpu.make_async_copy(loadings.at[j], held.at[j], loads.at[j])

    for j in range(lat_rows):
        load(j).start()
    barrier = pltpu.get_barrier_semaphore()
    for shift in range(1, n):
        peer = lax.rem(me + shift, n)
        pl.semaphore_signal(barrier, inc=1, device_id=(peer // n_lon, lax.rem(peer, n_lon)),
                            device_id_type=MESH)

    def rows_of(body, init):
        def step(i, carry):
            for k in range(unroll):
                carry = body(i * unroll + k, carry)
            return carry

        return lax.fori_loop(0, lat_rows // unroll, step, init)

    def normalise(j, colsq):
        load(j).wait()
        x = held[j]
        root = weights[1, lat * lat_rows + j]
        y = x * (root / jnp.sqrt(jnp.sum(x * x, axis=1, keepdims=True) + 1e-06))
        held[j] = y
        yh[j], yl[j] = split(y)
        return colsq + jnp.sum(y * y, axis=0, keepdims=True)

    none = jnp.zeros((1, modes), jnp.float32)
    colsq = rows_of(normalise, none)
    gram[...] = jnp.zeros_like(gram)
    cubic[...] = jnp.zeros_like(cubic)
    pl.semaphore_wait(barrier, n - 1)
    reduce1.spread(colsq)

    def first(i, carry):
        grams, cubics = [], []
        for k in range(unroll):
            j = i * unroll + k
            y = held[j]
            t_parts = split(y.T)
            th[j], tl[j] = t_parts
            inverse = weights[2, lat * lat_rows + j]
            grams.append(mm3(t_parts, (yh[j], yl[j])))
            cubics.append(mm3(t_parts, split(y * y * y * inverse)))
        gram[...] += sum(grams[1:], grams[0])
        cubic[...] += sum(cubics[1:], cubics[0])
        return carry

    lax.fori_loop(0, lat_rows // unroll, first, 0)
    colsq = reduce1.total(modes)
    local = cubic[...] - gram[...] * (colsq / total)
    src1[:, :, :modes] = local.reshape(owners, SUB, modes)
    reduce1.scatter()
    cubic[...] = jnp.zeros_like(cubic)
    reduce1.gather()
    rotation = polar(full1[:, :, :modes].reshape(modes, modes))
    r_parts = split(rotation)

    def spin(j, colsq):
        spun = mm3((yh[j], yl[j]), r_parts)
        held[j] = spun
        return colsq + jnp.sum(spun * spun, axis=0, keepdims=True)

    reduce2.spread(rows_of(spin, none))

    def second(i, carry):
        cubics = []
        for k in range(unroll):
            j = i * unroll + k
            spun = held[j]
            inverse = weights[2, lat * lat_rows + j]
            cubics.append(mm3((th[j], tl[j]), split(spun * spun * spun * inverse)))
        cubic[...] += sum(cubics[1:], cubics[0])
        return carry

    lax.fori_loop(0, lat_rows // unroll, second, 0)
    turned = mm3(split(gram[...]), r_parts)
    colsq = reduce2.total(modes)
    local = cubic[...] - turned * (colsq / total)
    src2[:, :, :modes] = local.reshape(owners, SUB, modes)
    reduce2.scatter()
    reduce2.gather()
    out[...] = polar(full2[:, :, :modes].reshape(modes, modes))


def latitude_weight(lat_total):
    rows = np.arange(lat_total, dtype=np.float32)
    degrees = np.float32(-90.0) + (rows + np.float32(0.5)) * np.float32(180.0 / lat_total)
    return np.cos(degrees * np.float32(math.pi / 180.0)).astype(np.float32)


def shards(n_lat, n_lon, loadings):
    lat_rows, lon_cols, modes = loadings.shape
    n = n_lat * n_lon
    owners = modes // SUB
    assert modes % SUB == 0 and owners <= n and modes <= LANES
    weights = latitude_weight(lat_rows * n_lat)
    total = float(np.sum(weights, dtype=np.float32) * np.float32(lon_cols * n_lon))
    table = jnp.asarray(np.stack([weights, np.sqrt(weights), 1.0 / weights]).astype(np.float32))
    f32, bf16 = jnp.float32, jnp.bfloat16

    bufs = [
        pltpu.VMEM((owners, SUB, LANES), f32),
        pltpu.VMEM((n, SUB, LANES), f32),
        pltpu.VMEM((owners, SUB, LANES), f32),
        pltpu.VMEM((n, 1, LANES), f32),
    ]

    rotation = pl.pallas_call(
        functools.partial(kernel, n_lat, n_lon, total),
        out_shape=jax.ShapeDtypeStruct((modes, modes), f32),
        in_specs=[
            pl.BlockSpec(memory_space=pltpu.SMEM),
            pl.BlockSpec(memory_space=pl.ANY),
        ],
        out_specs=pl.BlockSpec(memory_space=pltpu.VMEM),
        scratch_shapes=[
            pltpu.VMEM((lat_rows, lon_cols, modes), f32),
            pltpu.VMEM((lat_rows, lon_cols, modes), bf16),
            pltpu.VMEM((lat_rows, lon_cols, modes), bf16),
            pltpu.VMEM((lat_rows, modes, lon_cols), bf16),
            pltpu.VMEM((lat_rows, modes, lon_cols), bf16),
            pltpu.VMEM((modes, modes), f32),
            pltpu.VMEM((modes, modes), f32),
            *bufs,
            *bufs,
            pltpu.SemaphoreType.DMA((6, n)),
            pltpu.SemaphoreType.DMA((6, n)),
            pltpu.SemaphoreType.DMA((lat_rows,)),
        ],
        compiler_params=pltpu.CompilerParams(
            collective_id=0, has_side_effects=True, vmem_limit_bytes=60 * 1024 * 1024
        ),
    )(table, loadings)
    rotated = jnp.einsum("abk,kl->abl", loadings, rotation, precision=lax.Precision.HIGH)
    return (rotated, rotation)


def solution(mesh):
    return jax.shard_map(
        functools.partial(shards, mesh.shape["lat"], mesh.shape["lon"]),
        mesh=mesh,
        in_specs=(P("lat", "lon", None),),
        out_specs=(P("lat", "lon", None), P()),
        check_vma=False,
    )
```

```python
import functools
import math

import jax
import jax.numpy as jnp
import numpy as np
from jax import lax
from jax.experimental import pallas as pl
from jax.experimental.pallas import tpu as pltpu
from jax.sharding import PartitionSpec as P

SWEEPS = 2
NS_STEPS = 20
SUB = 8
LANES = 256
MESH = pl.DeviceIdType.MESH
NN = (((1,), (0,)), ((), ()))
NT = (((1,), (1,)), ((), ()))


def split(value):
    high = value.astype(jnp.bfloat16)
    low = (value - high.astype(jnp.float32)).astype(jnp.bfloat16)
    return high, low


def mm(left, right, dims=NN):
    return lax.dot_general(left, right, dims, preferred_element_type=jnp.float32)


def mm3(left, right, dims=NN):
    lh, ll = left
    rh, rl = right
    return mm(lh, rh, dims) + (mm(lh, rl, dims) + mm(ll, rh, dims))


def polar(gradient):
    squares = jnp.sum(gradient * gradient, axis=0, keepdims=True)
    norm = jnp.sqrt(jnp.sum(squares, axis=1, keepdims=True))

    def step(_, x):
        parts = split(x)
        inner = mm3(parts, parts, NT)
        return 1.5 * x - 0.5 * mm3(split(inner), parts)

    return lax.fori_loop(0, NS_STEPS, step, gradient / norm, unroll=4)


class Reduce:
    def __init__(self, me, n, n_lon, owners, bufs, sems):
        self.me, self.n, self.n_lon, self.owners = me, n, n_lon, owners
        self.src, self.got, self.full, self.rows = bufs
        self.sems = sems

    def copy(self, source, target, device, phase, sent, landed):
        return pltpu.make_async_remote_copy(
            src_ref=source,
            dst_ref=target,
            send_sem=self.sems.at[phase, sent],
            recv_sem=self.sems.at[phase + 1, landed],
            device_id=(device // self.n_lon, lax.rem(device, self.n_lon)),
            device_id_type=MESH,
        )

    def part(self, peer, source):
        return self.copy(self.src.at[peer], self.got.at[source], peer, 0, peer, source)

    def whole(self, peer, owner):
        return self.copy(self.full.at[owner], self.full.at[owner], peer, 2, peer, owner)

    def row(self, peer, source):
        return self.copy(self.rows.at[source], self.rows.at[source], peer, 4, peer, source)

    def spread(self, value):
        me, n = self.me, self.n
        self.rows[me, :, : value.shape[1]] = value
        for shift in range(1, n):
            self.row(lax.rem(me + shift, n), me).start()

    def total(self, width):
        me, n = self.me, self.n
        for shift in range(1, n):
            peer = lax.rem(me + n - shift, n)
            self.row(peer, peer).wait_recv()
        acc = self.rows[0]
        for source in range(1, n):
            acc = acc + self.rows[source]
        for shift in range(1, n):
            self.row(lax.rem(me + shift, n), me).wait_send()
        return acc[:, :width]

    def scatter(self):
        me, n = self.me, self.n
        for shift in range(1, n):
            peer = lax.rem(me + shift, n)

            @pl.when(peer < self.owners)
            def _():
                self.part(peer, me).start()

    def gather(self):
        me, n = self.me, self.n
        following = lax.rem(me + 1, n)

        @pl.when(me < self.owners)
        def _():
            acc = self.src[me]
            for shift in range(1, n):
                peer = lax.rem(me + n - shift, n)
                self.copy(self.src.at[me], self.got.at[peer], following, 0, peer, peer).wait_recv()
                acc = acc + self.got[peer]
            self.full[me] = acc
            for shift in range(1, n):
                self.whole(lax.rem(me + shift, n), me).start()

        for shift in range(1, n):
            peer = lax.rem(me + n - shift, n)

            @pl.when(peer < self.owners)
            def _():
                self.whole(following, peer).wait_recv()
                self.part(peer, me).wait_send()

        @pl.when(me < self.owners)
        def _():
            for shift in range(1, n):
                self.whole(lax.rem(me + shift, n), me).wait_send()


def kernel(n_lat, n_lon, total, weights, loadings, out, held, yh, yl, th, tl, gram, cubic,
           src1, got1, full1, rows1, src2, got2, full2, rows2, sems1, sems2, loads):
    lat_rows, lon_cols, modes = held.shape
    n = n_lat * n_lon
    owners = modes // SUB
    unroll = next(k for k in (11, 4, 3, 2, 1) if lat_rows % k == 0)
    lat, lon = lax.axis_index("lat"), lax.axis_index("lon")
    me = lat * n_lon + lon
    reduce1 = Reduce(me, n, n_lon, owners, (src1, got1, full1, rows1), sems1)
    reduce2 = Reduce(me, n, n_lon, owners, (src2, got2, full2, rows2), sems2)

    def load(j):
        return pltpu.make_async_copy(loadings.at[j], held.at[j], loads.at[j])

    for j in range(lat_rows):
        load(j).start()
    barrier = pltpu.get_barrier_semaphore()
    for shift in range(1, n):
        peer = lax.rem(me + shift, n)
        pl.semaphore_signal(barrier, inc=1, device_id=(peer // n_lon, lax.rem(peer, n_lon)),
                            device_id_type=MESH)

    def rows_of(body, init):
        def step(i, carry):
            for k in range(unroll):
                carry = body(i * unroll + k, carry)
            return carry

        return lax.fori_loop(0, lat_rows // unroll, step, init)

    def normalise(j, colsq):
        load(j).wait()
        x = held[j]
        root = weights[1, lat * lat_rows + j]
        y = x * (root / jnp.sqrt(jnp.sum(x * x, axis=1, keepdims=True) + 1e-06))
        held[j] = y
        yh[j], yl[j] = split(y)
        return colsq + jnp.sum(y * y, axis=0, keepdims=True)

    none = jnp.zeros((1, modes), jnp.float32)
    colsq = rows_of(normalise, none)
    gram[...] = jnp.zeros_like(gram)
    cubic[...] = jnp.zeros_like(cubic)
    pl.semaphore_wait(barrier, n - 1)
    reduce1.spread(colsq)

    def first(i, carry):
        grams, cubics = [], []
        for k in range(unroll):
            j = i * unroll + k
            y = held[j]
            t_parts = split(y.T)
            th[j], tl[j] = t_parts
            inverse = weights[2, lat * lat_rows + j]
            grams.append(mm3(t_parts, (yh[j], yl[j])))
            cubics.append(mm3(t_parts, split(y * y * y * inverse)))
        gram[...] += sum(grams[1:], grams[0])
        cubic[...] += sum(cubics[1:], cubics[0])
        return carry

    lax.fori_loop(0, lat_rows // unroll, first, 0)
    colsq = reduce1.total(modes)
    local = cubic[...] - gram[...] * (colsq / total)
    src1[:, :, :modes] = local.reshape(owners, SUB, modes)
    reduce1.scatter()
    cubic[...] = jnp.zeros_like(cubic)
    reduce1.gather()
    rotation = polar(full1[:, :, :modes].reshape(modes, modes))
    r_parts = split(rotation)

    def spin(j, colsq):
        spun = mm3((yh[j], yl[j]), r_parts)
        held[j] = spun
        return colsq + jnp.sum(spun * spun, axis=0, keepdims=True)

    reduce2.spread(rows_of(spin, none))

    def second(i, carry):
        cubics = []
        for k in range(unroll):
            j = i * unroll + k
            spun = held[j]
            inverse = weights[2, lat * lat_rows + j]
            cubics.append(mm3((th[j], tl[j]), split(spun * spun * spun * inverse)))
        cubic[...] += sum(cubics[1:], cubics[0])
        return carry

    lax.fori_loop(0, lat_rows // unroll, second, 0)
    turned = mm3(split(gram[...]), r_parts)
    colsq = reduce2.total(modes)
    local = cubic[...] - turned * (colsq / total)
    src2[:, :, :modes] = local.reshape(owners, SUB, modes)
    reduce2.scatter()
    reduce2.gather()
    out[...] = polar(full2[:, :, :modes].reshape(modes, modes))


def latitude_weight(lat_total):
    rows = np.arange(lat_total, dtype=np.float32)
    degrees = np.float32(-90.0) + (rows + np.float32(0.5)) * np.float32(180.0 / lat_total)
    return np.cos(degrees * np.float32(math.pi / 180.0)).astype(np.float32)


def shards(n_lat, n_lon, loadings):
    lat_rows, lon_cols, modes = loadings.shape
    n = n_lat * n_lon
    owners = modes // SUB
    assert modes % SUB == 0 and owners <= n and modes <= LANES
    weights = latitude_weight(lat_rows * n_lat)
    total = float(np.sum(weights, dtype=np.float32) * np.float32(lon_cols * n_lon))
    table = jnp.asarray(np.stack([weights, np.sqrt(weights), 1.0 / weights]).astype(np.float32))
    f32, bf16 = jnp.float32, jnp.bfloat16

    bufs = [
        pltpu.VMEM((owners, SUB, LANES), f32),
        pltpu.VMEM((n, SUB, LANES), f32),
        pltpu.VMEM((owners, SUB, LANES), f32),
        pltpu.VMEM((n, 1, LANES), f32),
    ]

    rotation = pl.pallas_call(
        functools.partial(kernel, n_lat, n_lon, total),
        out_shape=jax.ShapeDtypeStruct((modes, modes), f32),
        in_specs=[
            pl.BlockSpec(memory_space=pltpu.SMEM),
            pl.BlockSpec(memory_space=pl.ANY),
        ],
        out_specs=pl.BlockSpec(memory_space=pltpu.VMEM),
        scratch_shapes=[
            pltpu.VMEM((lat_rows, lon_cols, modes), f32),
            pltpu.VMEM((lat_rows, lon_cols, modes), bf16),
            pltpu.VMEM((lat_rows, lon_cols, modes), bf16),
            pltpu.VMEM((lat_rows, modes, lon_cols), bf16),
            pltpu.VMEM((lat_rows, modes, lon_cols), bf16),
            pltpu.VMEM((modes, modes), f32),
            pltpu.VMEM((modes, modes), f32),
            *bufs,
            *bufs,
            pltpu.SemaphoreType.DMA((6, n)),
            pltpu.SemaphoreType.DMA((6, n)),
            pltpu.SemaphoreType.DMA((lat_rows,)),
        ],
        compiler_params=pltpu.CompilerParams(
            collective_id=0, has_side_effects=True, vmem_limit_bytes=60 * 1024 * 1024
        ),
    )(table, loadings)
    rotated = jnp.einsum("abk,kl->abl", loadings, rotation, precision=lax.Precision.HIGH)
    return (rotated, rotation)


def solution(mesh):
    return jax.shard_map(
        functools.partial(shards, mesh.shape["lat"], mesh.shape["lon"]),
        mesh=mesh,
        in_specs=(P("lat", "lon", None),),
        out_specs=(P("lat", "lon", None), P()),
        check_vma=False,
    )
```
